512 devices in a mesh: batch: 64 (over z, y), cols: 8 (over x, core).
Axes of the slice: x: 4, y: 8, z: 8, core: 2. Of those that a mesh axis runs over, the one named last changes fastest.
Arguments:
- grad_up: float32 [64, 1024, 4096], P('batch', None, 'cols'), may hold values from -1.75 to 1.75
- grad_down: float32 [64, 4096, 1024], P('batch', 'cols'), may hold values from -1.75 to 1.75
- grad_query: float32 [64, 1024, 1024], P('batch', None, 'cols'), may hold values from -1.75 to 1.75
- grad_key: float32 [64, 1024, 1024], P('batch', None, 'cols'), may hold values from -1.75 to 1.75
- grad_value: float32 [64, 1024, 1024], P('batch', None, 'cols'), may hold values from -1.75 to 1.75
- grad_mixed: float32 [64, 1024, 1024], P('batch', 'cols'), may hold values from -1.75 to 1.75
- grad_norm: float32 [64, 1024], P('batch'), may hold values from -16 to 16
- weight_up: float32 [1024, 4096], P('batch', 'cols'), may hold values from -0.1875 to 0.1875
- weight_down: float32 [4096, 1024], P('cols', 'batch'), may hold values from -0.09375 to 0.09375
- weight_query: float32 [1024, 1024], P('batch', 'cols'), may hold values from -0.1875 to 0.1875
- weight_key: float32 [1024, 1024], P('batch', 'cols'), may hold values from -0.1875 to 0.1875
- weight_value: float32 [1024, 1024], P('batch', 'cols'), may hold values from -0.1875 to 0.1875
- weight_mixed: float32 [1024, 1024], P('cols', 'batch'), may hold values from -0.1875 to 0.1875
- weight_norm: float32 [1024], P('batch'), may hold values from 0.25 to 1.75
Outputs:
- copy_up: bfloat16 [1024, 4096], P(None, 'cols')
- copy_down: bfloat16 [4096, 1024], P('cols')
- copy_query: bfloat16 [1024, 1024], P(None, 'cols')
- copy_key: bfloat16 [1024, 1024], P(None, 'cols')
- copy_value: bfloat16 [1024, 1024], P(None, 'cols')
- copy_mixed: bfloat16 [1024, 1024], P('cols')
- copy_norm: bfloat16 [1024], replicated
- new_up: float32 [1024, 4096], P('batch', 'cols')
- new_down: float32 [4096, 1024], P('cols', 'batch')
- new_query: float32 [1024, 1024], P('batch', 'cols')
- new_key: float32 [1024, 1024], P('batch', 'cols')
- new_value: float32 [1024, 1024], P('batch', 'cols')
- new_mixed: float32 [1024, 1024], P('cols', 'batch')
- new_norm: float32 [1024], P('batch')
The draws below stay inside these ranges and needn't reach their ends.
All inputs are finite; a program needn't handle non-finite values.
Results may differ from the reference program's by a relative error of at most 0.0004.
Values may be sent and summed in bfloat16 or wider, within the bound.
No kernel may reach another device: no remote copies, remote signals or barrier semaphores. Data moves between devices by JAX's collectives and lax.ppermute only.
A program may use at most 64 MiB of HBM per device.

```python
import jax
import jax.numpy as jnp

WIDTH = 1024
INNER = 4096
ATTN = 1024
REPLICAS = 64


def strengthened(array, own_key, source, target, blocks, factor):
    def block_of(dim):
        return (jnp.arange(array.shape[dim]) // (array.shape[dim] // blocks)).reshape((-1,) + (1,) * (array.ndim - 1 - dim))

    first = jax.random.permutation(own_key, blocks)[block_of(target)]
    far = (block_of(target) + blocks // 2) % blocks
    return jnp.where((block_of(source) == first) | (block_of(source) == far), factor * array, array)


def shard_levels(key, dims, cuts, least, top_value):
    def one(position, shards_of):
        steps = jax.random.uniform(jax.random.fold_in(jax.random.fold_in(key, 6), position), (shards_of,), jnp.float32, least / len(cuts), top_value / len(cuts))
        return jnp.repeat(jnp.exp(steps), dims[position] // shards_of).reshape((-1,) + (1,) * (len(dims) - position - 1))

    loudness = one(*cuts[0])
    for cut in cuts[1:]:
        loudness = loudness * one(*cut)
    return loudness


def gaussian(stream_key, dims, width, limit, pieces=(), dtype=jnp.bfloat16):
    factor_of = shard_levels(stream_key, dims, pieces, -0.22, 0.18) if pieces else 1.0
    result = jax.random.normal(stream_key, dims, jnp.float32) * width * factor_of
    return jnp.minimum(jnp.maximum(result, -limit), limit).astype(dtype)


def noise_with(own_key, shape, spread, reach, cuts, heavy, held_as=jnp.bfloat16):
    array = spread * jax.random.normal(own_key, shape, jnp.float32)
    if cuts:
        array = array * shard_levels(own_key, shape, cuts, -0.22, 0.18)
    return jnp.clip(strengthened(array, jax.random.fold_in(own_key, 3), *heavy), -reach, reach).astype(held_as)


def setup_inputs(seed: int = 0) -> dict:
    key_of = jax.random.split(jax.random.key(seed), 15)
    grad_up = noise_with(key_of[0], (REPLICAS, WIDTH, INNER), 0.1, 1.75, ((0, 64), (2, 8)), (0, 1, 64, 4.0), jnp.float32)
    grad_down = noise_with(key_of[1], (REPLICAS, INNER, WIDTH), 0.1, 1.75, ((0, 64), (1, 8)), (0, 2, 64, 4.0), jnp.float32)
    grad_query = noise_with(key_of[2], (REPLICAS, WIDTH, ATTN), 0.1, 1.75, ((0, 64), (2, 8)), (0, 1, 64, 4.0), jnp.float32)
    grad_key = noise_with(key_of[3], (REPLICAS, WIDTH, ATTN), 0.1, 1.75, ((0, 64), (2, 8)), (0, 1, 64, 4.0), jnp.float32)
    grad_value = noise_with(key_of[4], (REPLICAS, WIDTH, ATTN), 0.1, 1.75, ((0, 64), (2, 8)), (0, 1, 64, 4.0), jnp.float32)
    grad_mixed = noise_with(key_of[5], (REPLICAS, ATTN, WIDTH), 0.1, 1.75, ((0, 64), (1, 8)), (0, 2, 64, 4.0), jnp.float32)
    grad_norm = noise_with(key_of[6], (REPLICAS, WIDTH), 1.0, 16.0, ((0, 64),), (0, 1, 64, 4.0), jnp.float32)
    weight_up = gaussian(key_of[7], (WIDTH, INNER), WIDTH ** -0.5, 0.1875, ((0, 64), (1, 8)), jnp.float32)
    weight_down = gaussian(key_of[8], (INNER, WIDTH), INNER ** -0.5, 0.09375, ((0, 8), (1, 64)), jnp.float32)
    weight_query = gaussian(key_of[9], (WIDTH, ATTN), WIDTH ** -0.5, 0.1875, ((0, 64), (1, 8)), jnp.float32)
    weight_key = gaussian(key_of[10], (WIDTH, ATTN), WIDTH ** -0.5, 0.1875, ((0, 64), (1, 8)), jnp.float32)
    weight_value = gaussian(key_of[11], (WIDTH, ATTN), WIDTH ** -0.5, 0.1875, ((0, 64), (1, 8)), jnp.float32)
    weight_mixed = gaussian(key_of[12], (ATTN, WIDTH), ATTN ** -0.5, 0.1875, ((0, 8), (1, 64)), jnp.float32)
    weight_norm = jnp.clip(1.0 + 0.15 * jax.random.normal(key_of[13], (WIDTH,), jnp.float32), 0.25, 1.75)
    return {"grad_up": grad_up, "grad_down": grad_down, "grad_query": grad_query, "grad_key": grad_key, "grad_value": grad_value, "grad_mixed": grad_mixed, "grad_norm": grad_norm, "weight_up": weight_up, "weight_down": weight_down, "weight_query": weight_query, "weight_key": weight_key, "weight_value": weight_value, "weight_mixed": weight_mixed, "weight_norm": weight_norm}


learn_rate = 0.3


def reference(grad_up, grad_down, grad_query, grad_key, grad_value, grad_mixed, grad_norm, weight_up, weight_down, weight_query, weight_key, weight_value, weight_mixed, weight_norm):
    mean_up = jnp.sum(grad_up.astype(jnp.float32), axis=0) * REPLICAS ** -0.5
    mean_down = jnp.sum(grad_down.astype(jnp.float32), axis=0) * REPLICAS ** -0.5
    mean_query = jnp.sum(grad_query.astype(jnp.float32), axis=0) * REPLICAS ** -0.5
    mean_key = jnp.sum(grad_key.astype(jnp.float32), axis=0) * REPLICAS ** -0.5
    mean_value = jnp.sum(grad_value.astype(jnp.float32), axis=0) * REPLICAS ** -0.5
    mean_mixed = jnp.sum(grad_mixed.astype(jnp.float32), axis=0) * REPLICAS ** -0.5
    mean_norm = jnp.sum(grad_norm.astype(jnp.float32), axis=0) * REPLICAS ** -0.5
    new_up = weight_up - learn_rate * mean_up
    new_down = weight_down - learn_rate * mean_down
    new_query = weight_query - learn_rate * mean_query
    new_key = weight_key - learn_rate * mean_key
    new_value = weight_value - learn_rate * mean_value
    new_mixed = weight_mixed - learn_rate * mean_mixed
    new_norm = weight_norm - learn_rate * mean_norm
    copy_up = new_up.astype(jnp.bfloat16)
    copy_down = new_down.astype(jnp.bfloat16)
    copy_query = new_query.astype(jnp.bfloat16)
    copy_key = new_key.astype(jnp.bfloat16)
    copy_value = new_value.astype(jnp.bfloat16)
    copy_mixed = new_mixed.astype(jnp.bfloat16)
    copy_norm = new_norm.astype(jnp.bfloat16)
    return copy_up, copy_down, copy_query, copy_key, copy_value, copy_mixed, copy_norm, new_up, new_down, new_query, new_key, new_value, new_mixed, new_norm
```

```python
import jax
import jax.numpy as jnp
from jax import lax
from jax.experimental import pallas as pl
from jax.experimental.pallas import tpu as pltpu
from jax.sharding import PartitionSpec as P

learn_rate = 0.3
AX = ("batch", "cols")
N = 8
T = 12
ROWS = T * 128 + 8
PART = T * 16 + 8
anywhere = pl.BlockSpec(memory_space=pl.ANY)
in_vmem = pl.BlockSpec(memory_space=pltpu.VMEM)


def groups(swap):
    found = []
    for c in range(8):
        for o in range(N):
            along_y = (c % 2 == 0) != swap
            found.append([((o * N + k) if along_y else (k * N + o)) * 8 + c for k in range(N)])
    return found


def exchange(x, swap):
    return lax.all_to_all(x, AX, 0, 0, axis_index_groups=groups(swap))


def core():
    return lax.axis_index("cols") % 2


def pack_body(up, down, q, k, v, mixed, norm, out, down_v, mixed_v, sems, tsems):
    c = core()
    loads = [
        pltpu.make_async_copy(down, down_v, tsems.at[0]),
        pltpu.make_async_copy(mixed, mixed_v, tsems.at[1]),
    ]
    for one in loads:
        one.start()

    def copies(first):
        for f in range(N):
            at = 0
            for a in (up, q, k, v):
                for t in range(a.shape[-1] // 128):
                    lanes = pl.ds(t * 128, 128)
                    src = a.at[:, f, :, lanes] if first else a.at[f, :, :, lanes]
                    row = (at if a is up else at + 4) * 128
                    yield pltpu.make_async_copy(src, out.at[f, pl.ds(row, 128)].reshape(N, 16, 128), sems)
                    at += 1

    @pl.when(c == 0)
    def _():
        for one in copies(True):
            one.start()

    @pl.when(c == 1)
    def _():
        for one in copies(False):
            one.start()

    out[:, T * 128 :, :] = norm[...]
    for one in loads:
        one.wait()
    for src, t0, n in ((down_v, 4, 4), (mixed_v, 11, 1)):
        for z in range(N):
            for t in range(n):
                tile = src[t * 128 : (t + 1) * 128, z * 128 : (z + 1) * 128].T
                for y in range(N):
                    f = jnp.where(c == 0, y, z)
                    s = jnp.where(c == 0, z, y)
                    row = pl.multiple_of((t0 + t) * 128 + s * 16, 16)
                    out[f, pl.ds(row, 16), :] = tile[y * 16 : (y + 1) * 16]

    for one in copies(False):
        one.wait()


def pack(up, down, q, k, v, mixed, norm):
    split = [a.reshape(N, N, 16, a.shape[-1]) for a in (up, q, k, v)]
    return pl.pallas_call(
        pack_body,
        name="pack",
        out_shape=jax.ShapeDtypeStruct((N, ROWS, 128), jnp.float32),
        in_specs=[anywhere] * 6 + [in_vmem],
        out_specs=in_vmem,
        scratch_shapes=[
            pltpu.VMEM(down.shape, jnp.float32),
            pltpu.VMEM(mixed.shape, jnp.float32),
            pltpu.SemaphoreType.DMA,
            pltpu.SemaphoreType.DMA((2,)),
        ],
    )(split[0], down, *split[1:], mixed, norm)


def middle_body(got, out):
    for t in range(T):
        rows = pl.ds(t * 128, 128)
        total = got[0, rows]
        for f in range(1, N):
            total += got[f, rows]
        out[:, t * 16 : (t + 1) * 16, :] = total.reshape(N, 16, 128)
    norm = got[0, T * 128 :]
    for f in range(1, N):
        norm += got[f, T * 128 :]
    out[:, T * 16 :, :] = jnp.broadcast_to(norm[:, None, :], (N, 8, 128))


def middle(got):
    return pl.pallas_call(
        middle_body,
        name="middle",
        out_shape=jax.ShapeDtypeStruct((N, PART, 128), jnp.float32),
        in_specs=[in_vmem],
        out_specs=in_vmem,
    )(got)


def update_body(rate, got, up, down, q, k, v, mixed, norm, n_up, n_down, n_q, n_k, n_v, n_mixed, n_norm, copies):
    def step(t, weight):
        rows = pl.ds(t * 16, 16)
        total = got[0, rows]
        for s in range(1, N):
            total += got[s, rows]
        new = weight - learn_rate * (total * rate)
        copies[:, rows] = jnp.broadcast_to(new.astype(jnp.bfloat16)[None], (N, 16, 128))
        return new

    for t in range(4):
        lanes = slice(t * 128, (t + 1) * 128)
        n_up[:, lanes] = step(t, up[:, lanes])
        n_down[lanes, :] = step(4 + t, down[lanes, :].T).T
    n_q[...] = step(8, q[...])
    n_k[...] = step(9, k[...])
    n_v[...] = step(10, v[...])
    n_mixed[...] = step(11, mixed[...].T).T
    total = got[0, T * 16 :]
    for s in range(1, N):
        total += got[s, T * 16 :]
    new = norm[...] - learn_rate * (total * rate)
    n_norm[...] = new
    copies[:, T * 16 :] = jnp.broadcast_to(new.astype(jnp.bfloat16)[None], (N, 8, 128))


def update(got, weights):
    shapes = [jax.ShapeDtypeStruct(w.shape, jnp.float32) for w in weights]
    rate = REPLICAS_RATE
    return pl.pallas_call(
        lambda *refs: update_body(rate, *refs),
        name="update",
        out_shape=shapes + [jax.ShapeDtypeStruct((N, PART, 128), jnp.bfloat16)],
        in_specs=[in_vmem] * 8,
        out_specs=[in_vmem] * 8,
    )(got, *weights)


REPLICAS_RATE = 64 ** (-0.5)


def unpack_body(got, up, down, q, k, v, mixed, got_v, sems, tsem):
    c = core()
    load = pltpu.make_async_copy(got, got_v, tsem)
    load.start()

    def copies(first):
        for f in range(N):
            for a, t0 in ((up, 0), (q, 8), (k, 9), (v, 10)):
                for t in range(a.shape[-1] // 128):
                    lanes = pl.ds(t * 128, 128)
                    dst = a.at[:, f, :, lanes] if first else a.at[f, :, :, lanes]
                    yield pltpu.make_async_copy(got.at[f, :, pl.ds((t0 + t) * 16, 16)], dst, sems)

    @pl.when(c == 0)
    def _():
        for one in copies(True):
            one.start()

    @pl.when(c == 1)
    def _():
        for one in copies(False):
            one.start()

    load.wait()
    for dst, t0, n in ((down, 4, 4), (mixed, 11, 1)):
        for z in range(N):
            for t in range(n):
                rows = pl.ds((t0 + t) * 16, 16)
                parts = [got_v[jnp.where(c == 0, y, z), jnp.where(c == 0, z, y), rows] for y in range(N)]
                dst[t * 128 : (t + 1) * 128, z * 128 : (z + 1) * 128] = jnp.concatenate(parts).T

    for one in copies(False):
        one.wait()


def unpack(got):
    def out(*shape):
        return jax.ShapeDtypeStruct(shape, jnp.bfloat16)

    up, down, q, k, v, mixed = pl.pallas_call(
        unpack_body,
        name="unpack",
        out_shape=[out(N, N, 16, 512), out(512, 1024)] + [out(N, N, 16, 128)] * 3 + [out(128, 1024)],
        in_specs=[anywhere],
        out_specs=[anywhere, in_vmem] + [anywhere] * 3 + [in_vmem],
        scratch_shapes=[pltpu.VMEM(got.shape, jnp.bfloat16), pltpu.SemaphoreType.DMA, pltpu.SemaphoreType.DMA],
    )(got)
    flat = [a.reshape(1024, -1) for a in (up, q, k, v)]
    return flat[0], down, *flat[1:], mixed


def by_core(x):
    return jnp.where(core() == 0, jnp.swapaxes(x, 0, 1), x)


def shards(g_up, g_down, g_q, g_k, g_v, g_mixed, g_norm, up, down, q, k, v, mixed, norm):
    tile = jnp.pad(by_core(g_norm[0].reshape(N, N, 16)), ((0, 0), (0, 0), (0, 112)))
    chunks = pack(g_up[0], g_down[0], g_q[0], g_k[0], g_v[0], g_mixed[0], tile)
    got = exchange(middle(exchange(chunks, False)), True)
    norm_tile = jnp.broadcast_to(jnp.pad(norm, (0, 112)), (8, 128))
    *new, mine = update(got, (up, down, q, k, v, mixed, norm_tile))
    near = exchange(mine, True)
    whole = exchange(jnp.broadcast_to(near[None], (N, *near.shape)), False)
    copies = unpack(whole)
    copy_norm = by_core(whole[:, :, T * 16, :16]).reshape(1024)
    return (*copies, copy_norm, *new[:6], new[6][0, :16])


def solution(mesh):
    placed = (
        P("batch", None, "cols"),
        P("batch", "cols", None),
        P("batch", None, "cols"),
        P("batch", None, "cols"),
        P("batch", None, "cols"),
        P("batch", "cols", None),
        P("batch", None),
        P("batch", "cols"),
        P("cols", "batch"),
        P("batch", "cols"),
        P("batch", "cols"),
        P("batch", "cols"),
        P("cols", "batch"),
        P("batch"),
    )
    whole = (P(None, "cols"), P("cols", None), P(None, "cols"), P(None, "cols"), P(None, "cols"), P("cols", None), P())
    return jax.shard_map(shards, mesh=mesh, in_specs=placed, out_specs=whole + placed[7:], check_vma=False)
```

```python
import jax
import jax.numpy as jnp
from jax import lax
from jax.experimental import pallas as pl
from jax.experimental.pallas import tpu as pltpu
from jax.sharding import PartitionSpec as P

learn_rate = 0.3
AX = ("batch", "cols")
N = 8
T = 12
ROWS = T * 128 + 8
PART = T * 16 + 8
in_hbm = pl.BlockSpec(memory_space=pltpu.MemorySpace.HBM)
in_vmem = pl.BlockSpec(memory_space=pltpu.VMEM)
mean_rate = 64 ** (-0.5)
HALF = 6 * 128


def groups(swap):
    found = []
    for c in range(8):
        for o in range(N):
            along_y = (c % 2 == 0) != swap
            found.append([((o * N + k) if along_y else (k * N + o)) * 8 + c for k in range(N)])
    return found


def exchange(x, swap):
    return lax.all_to_all(x, AX, 0, 0, axis_index_groups=groups(swap))


def shift(x, by):
    pairs = []
    for group in groups(False):
        pairs += [(group[k], group[(k + by) % N]) for k in range(N)]
    return lax.ppermute(x, AX, sorted(pairs))


def place():
    c = lax.axis_index("cols") % 2
    b = lax.axis_index("batch")
    z, y = b // N, b % N
    return c, jnp.where(c == 0, y, z), jnp.where(c == 0, z, y)


def pack_body(up, down, q, k, v, mixed, norm, own, p1, m1, p2, m2, p3, m3, h0, h1, down_v, mixed_v, turned, sems, tsems):
    c, pos, _ = place()
    loads = [
        pltpu.make_async_copy(down, down_v, tsems.at[0]),
        pltpu.make_async_copy(mixed, mixed_v, tsems.at[1]),
    ]
    for one in loads:
        one.start()
    chunks = {0: own, 1: p1, -1: m1, 2: p2, -2: m2, 3: p3, -3: m3}

    def target(d, t):
        if d == 4:
            return h0.at[pl.ds(t * 128, 128)] if t < 6 else h1.at[pl.ds((t - 6) * 128, 128)]
        return chunks[d].at[pl.ds(t * 128, 128)]

    def copies(first):
        for d in range(-3, 5):
            f = (pos + d + N) % N
            for a, t0 in ((up, 0), (q, 8), (k, 9), (v, 10)):
                for t in range(a.shape[-1] // 128):
                    lanes = pl.ds(t * 128, 128)
                    src = a.at[:, f, :, lanes] if first else a.at[f, :, :, lanes]
                    yield pltpu.make_async_copy(src, target(d, t0 + t).reshape(N, 16, 128), sems)

    @pl.when(c == 0)
    def _():
        for one in copies(True):
            one.start()

    @pl.when(c == 1)
    def _():
        for one in copies(False):
            one.start()

    for d in range(-3, 4):
        chunks[d][T * 128 :, :] = norm[...]
    h1[T * 128 - HALF :, :] = norm[...]
    for one in loads:
        one.wait()
    for src, t0, n in ((down_v, 0, 4), (mixed_v, 4, 1)):
        for z in range(N):
            for t in range(n):
                tile = src[t * 128 : (t + 1) * 128, z * 128 : (z + 1) * 128].T
                turned[t0 + t, z] = tile.reshape(N, 16, 128)
    for d in range(-3, 5):
        f = (pos + d + N) % N
        for t in range(5):
            into = target(d, (4, 5, 6, 7, 11)[t])
            for s in range(N):
                into[s * 16 : (s + 1) * 16] = turned[t, jnp.where(c == 0, s, f), jnp.where(c == 0, f, s)]

    for one in copies(False):
        one.wait()


def pack(up, down, q, k, v, mixed, norm):
    split = [a.reshape(N, N, 16, a.shape[-1]) for a in (up, q, k, v)]
    lines = [ROWS] * 7 + [HALF, ROWS - HALF]
    return pl.pallas_call(
        pack_body,
        name="pack",
        compiler_params=pltpu.CompilerParams(vmem_limit_bytes=54 << 20),
        out_shape=[pltpu.VMEM((n, 128), jnp.float32) for n in lines],
        in_specs=[in_hbm] * 6 + [in_vmem],
        out_specs=[in_vmem] * 9,
        scratch_shapes=[
            pltpu.VMEM(down.shape, jnp.float32),
            pltpu.VMEM(mixed.shape, jnp.float32),
            pltpu.VMEM((5, N, N, 16, 128), jnp.float32),
            pltpu.SemaphoreType.DMA,
            pltpu.SemaphoreType.DMA((2,)),
        ],
    )(split[0], down, *split[1:], mixed, norm)


def merge_body(p2, m2, far_p, far_m, half_p, half_m, to_p, to_m):
    to_p[:HALF] = p2[:HALF] + far_p[:HALF] + half_p[...]
    to_p[HALF:] = p2[HALF:] + far_p[HALF:]
    to_m[:HALF] = m2[:HALF] + far_m[:HALF]
    to_m[HALF:] = m2[HALF:] + far_m[HALF:] + half_m[...]


def merge(*parts):
    return pl.pallas_call(
        merge_body,
        name="merge",
        compiler_params=pltpu.CompilerParams(vmem_limit_bytes=12 << 20),
        out_shape=[jax.ShapeDtypeStruct((ROWS, 128), jnp.float32)] * 2,
        in_specs=[in_vmem] * 6,
        out_specs=[in_vmem] * 2,
    )(*parts)


def middle_body(own, a, b, c, d, out):
    for t in range(T):
        rows = pl.ds(t * 128, 128)
        total = (own[rows] + a[rows]) + (b[rows] + c[rows]) + d[rows]
        out[:, t * 16 : (t + 1) * 16, :] = total.reshape(N, 16, 128)
    rows = pl.ds(T * 128, 8)
    norm = (own[rows] + a[rows]) + (b[rows] + c[rows]) + d[rows]
    out[:, T * 16 :, :] = jnp.broadcast_to(norm[None], (N, 8, 128))


def middle(*parts):
    return pl.pallas_call(
        middle_body,
        name="middle",
        compiler_params=pltpu.CompilerParams(vmem_limit_bytes=10 << 20),
        out_shape=jax.ShapeDtypeStruct((N, PART, 128), jnp.float32),
        in_specs=[in_vmem] * 5,
        out_specs=in_vmem,
    )(*parts)


def update_body(got, up, down, q, k, v, mixed, norm, n_up, n_down, n_q, n_k, n_v, n_mixed, n_norm, copies):
    def step(t, weight):
        rows = pl.ds(t * 16, 16)
        total = got[0, rows]
        for s in range(1, N):
            total += got[s, rows]
        new = weight - learn_rate * (total * mean_rate)
        copies[:, rows] = jnp.broadcast_to(new.astype(jnp.bfloat16)[None], (N, 16, 128))
        return new

    for t in range(4):
        lanes = slice(t * 128, (t + 1) * 128)
        n_up[:, lanes] = step(t, up[:, lanes])
        n_down[:, lanes] = step(4 + t, down[:, lanes])
    n_q[...] = step(8, q[...])
    n_k[...] = step(9, k[...])
    n_v[...] = step(10, v[...])
    n_mixed[...] = step(11, mixed[...])
    total = got[0, T * 16 :]
    for s in range(1, N):
        total += got[s, T * 16 :]
    b = lax.axis_index("batch")
    z, y = b // N, b % N
    weight = pltpu.roll(norm[...], y * 16, 1)
    new = weight - learn_rate * (total * mean_rate)
    new = jnp.where(lax.broadcasted_iota(jnp.int32, (8, 128), 0) == z, new, 0.0)
    new = jnp.where(lax.broadcasted_iota(jnp.int32, (8, 128), 1) // 16 == y, new, 0.0)
    n_norm[...] = pltpu.roll(jnp.broadcast_to(jnp.sum(new, axis=0, keepdims=True), (8, 128)), 128 - y * 16, 1)
    copies[:, T * 16 :] = jnp.broadcast_to(new.astype(jnp.bfloat16)[None], (N, 8, 128))


def update(got, weights):
    shapes = [jax.ShapeDtypeStruct(w.shape, jnp.float32) for w in weights]
    return pl.pallas_call(
        update_body,
        name="update",
        compiler_params=pltpu.CompilerParams(vmem_limit_bytes=6 << 20),
        out_shape=shapes + [jax.ShapeDtypeStruct((N, PART, 128), jnp.bfloat16)],
        in_specs=[in_vmem] * 8,
        out_specs=[in_vmem] * 8,
    )(got, *weights)


def unpack_body(own, a1, b1, a2, b2, a3, b3, h0, h1, up, down, q, k, v, mixed, norm, turned):
    c, pos, _ = place()
    chunks = {0: own, -1: a1, 1: b1, -2: a2, 2: b2, -3: a3, 3: b3}
    total = jnp.zeros((8, 128), jnp.float32)
    for d in range(-3, 5):
        f = (pos + d + N) % N
        for s in range(N):
            src, at = (chunks[d], s * PART) if d < 4 else (h0, s * PART) if s < 4 else (h1, (s - 4) * PART)
            z, y = jnp.where(c == 0, s, f), jnp.where(c == 0, f, s)
            for t in range(T):
                block = src[at + t * 16 : at + (t + 1) * 16]
                if t < 4:
                    up[z, y, :, t * 128 : (t + 1) * 128] = block
                elif t < 8 or t == 11:
                    turned[t - 4 if t < 8 else 4, z, y] = block
                else:
                    (q, k, v)[t - 8][z, y] = block
            total += src[at + T * 16 : at + PART].astype(jnp.float32)
    norm[...] = total.astype(jnp.bfloat16)
    for dst, t0, n in ((down, 0, 4), (mixed, 4, 1)):
        for z in range(N):
            for t in range(n):
                dst[t * 128 : (t + 1) * 128, z * 128 : (z + 1) * 128] = turned[t0 + t, z].reshape(128, 128).T


def unpack(*chunks):
    def out(*shape):
        return jax.ShapeDtypeStruct(shape, jnp.bfloat16)

    up, down, q, k, v, mixed, norm = pl.pallas_call(
        unpack_body,
        name="unpack",
        compiler_params=pltpu.CompilerParams(vmem_limit_bytes=16 << 20),
        out_shape=[out(N, N, 16, 512), out(512, 1024)] + [out(N, N, 16, 128)] * 3 + [out(128, 1024), out(8, 128)],
        in_specs=[in_vmem] * 9,
        out_specs=[in_vmem] * 7,
        scratch_shapes=[pltpu.VMEM((5, N, N, 16, 128), jnp.bfloat16)],
    )(*chunks)
    flat = [a.reshape(1024, -1) for a in (up, q, k, v)]
    return flat[0], down, *flat[1:], mixed, norm.reshape(1024)


def summed(chunks):
    own, p1, m1, p2, m2, p3, m3, h0, h1 = chunks
    far_p, far_m = shift(p3, 1), shift(m3, -1)
    half_p, half_m = shift(h0, 2), shift(h1, -2)
    near_p, near_m = shift(p1, 1), shift(m1, -1)
    to_p, to_m = merge(p2, m2, far_p, far_m, half_p, half_m)
    return middle(own, near_p, near_m, shift(to_p, 2), shift(to_m, -2))


def spread(own):
    half = own.shape[0] // 2
    a2, b2 = shift(own, 2), shift(own, -2)
    a1, b1 = shift(own, 1), shift(own, -1)
    a3, b3 = shift(a2, 1), shift(b2, -1)
    h0, h1 = shift(a2[:half], 2), shift(b2[half:], -2)
    return own, a1, b1, a2, b2, a3, b3, h0, h1


def shards(g_up, g_down, g_q, g_k, g_v, g_mixed, g_norm, up, down, q, k, v, mixed, norm):
    chunks = pack(g_up[0], g_down[0], g_q[0], g_k[0], g_v[0], g_mixed[0], g_norm.reshape(8, 128))
    norm_tile = jnp.broadcast_to(jnp.pad(norm, (0, 112)), (8, 128))
    parts, norm_tile = lax.optimization_barrier((summed(chunks), norm_tile))
    got = exchange(parts, True)
    *new, mine = update(got, (up, down.T, q, k, v, mixed.T, norm_tile))
    copies = unpack(*spread(exchange(mine, True).reshape(N * PART, 128)))
    n_up, n_down, n_q, n_k, n_v, n_mixed, n_norm = new
    return (*copies, n_up, n_down.T, n_q, n_k, n_v, n_mixed.T, n_norm[0, :16])


def solution(mesh):
    placed = (
        P("batch", None, "cols"),
        P("batch", "cols", None),
        P("batch", None, "cols"),
        P("batch", None, "cols"),
        P("batch", None, "cols"),
        P("batch", "cols", None),
        P("batch", None),
        P("batch", "cols"),
        P("cols", "batch"),
        P("batch", "cols"),
        P("batch", "cols"),
        P("batch", "cols"),
        P("cols", "batch"),
        P("batch"),
    )
    whole = (P(None, "cols"), P("cols", None), P(None, "cols"), P(None, "cols"), P(None, "cols"), P("cols", None), P())
    return jax.shard_map(shards, mesh=mesh, in_specs=placed, out_specs=whole + placed[7:], check_vma=False)
```

```python
import functools

import jax
import jax.numpy as jnp
from jax import lax
from jax.experimental import pallas as pl
from jax.experimental.pallas import tpu as pltpu
from jax.sharding import PartitionSpec as P

learn_rate = 0.3
AX = ("batch", "cols")
N = 8
T = 12
ROWS = T * 128 + 8
PART = T * 16 + 8
in_hbm = pl.BlockSpec(memory_space=pltpu.MemorySpace.HBM)
in_vmem = pl.BlockSpec(memory_space=pltpu.VMEM)
mean_rate = 64 ** (-0.5)
HALF = 6 * 128


def groups(swap):
    found = []
    for c in range(8):
        for o in range(N):
            along_y = (c % 2 == 0) != swap
            found.append([((o * N + k) if along_y else (k * N + o)) * 8 + c for k in range(N)])
    return found


def exchange(x, swap):
    return lax.all_to_all(x, AX, 0, 0, axis_index_groups=groups(swap))


def shift(x, by):
    pairs = []
    for group in groups(False):
        pairs += [(group[k], group[(k + by) % N]) for k in range(N)]
    return lax.ppermute(x, AX, sorted(pairs))


def place():
    c = lax.axis_index("cols") % 2
    b = lax.axis_index("batch")
    z, y = b // N, b % N
    return c, jnp.where(c == 0, y, z), jnp.where(c == 0, z, y)


def pack_body(up, down, q, k, v, mixed, norm, own, p1, m1, p2, m2, p3, m3, h0, h1, down_v, mixed_v, turned, sems, tsems):
    c, pos, _ = place()
    loads = [
        pltpu.make_async_copy(down, down_v, tsems.at[0]),
        pltpu.make_async_copy(mixed, mixed_v, tsems.at[1]),
    ]
    for one in loads:
        one.start()
    chunks = {0: own, 1: p1, -1: m1, 2: p2, -2: m2, 3: p3, -3: m3}

    def target(d, t):
        if d == 4:
            return h0.at[pl.ds(t * 128, 128)] if t < 6 else h1.at[pl.ds((t - 6) * 128, 128)]
        return chunks[d].at[pl.ds(t * 128, 128)]

    def copies(first):
        for d in range(-3, 5):
            f = (pos + d + N) % N
            for a, t0 in ((up, 0), (q, 8), (k, 9), (v, 10)):
                for t in range(a.shape[-1] // 128):
                    lanes = pl.ds(t * 128, 128)
                    src = a.at[:, f, :, lanes] if first else a.at[f, :, :, lanes]
                    yield pltpu.make_async_copy(src, target(d, t0 + t).reshape(N, 16, 128), sems)

    @pl.when(c == 0)
    def _():
        for one in copies(True):
            one.start()

    @pl.when(c == 1)
    def _():
        for one in copies(False):
            one.start()

    for d in range(-3, 4):
        chunks[d][T * 128 :, :] = norm[...]
    h1[T * 128 - HALF :, :] = norm[...]
    for one in loads:
        one.wait()
    for src, t0, n in ((down_v, 0, 4), (mixed_v, 4, 1)):
        for z in range(N):
            for t in range(n):
                tile = src[t * 128 : (t + 1) * 128, z * 128 : (z + 1) * 128].T
                turned[t0 + t, z] = tile.reshape(N, 16, 128)
    for d in range(-3, 5):
        f = (pos + d + N) % N
        for t in range(5):
            into = target(d, (4, 5, 6, 7, 11)[t])
            for s in range(N):
                into[s * 16 : (s + 1) * 16] = turned[t, jnp.where(c == 0, s, f), jnp.where(c == 0, f, s)]

    for one in copies(False):
        one.wait()


def pack(up, down, q, k, v, mixed, norm):
    split = [a.reshape(N, N, 16, a.shape[-1]) for a in (up, q, k, v)]
    lines = [ROWS] * 7 + [HALF, ROWS - HALF]
    return pl.pallas_call(
        pack_body,
        name="pack",
        compiler_params=pltpu.CompilerParams(vmem_limit_bytes=54 << 20),
        out_shape=[pltpu.VMEM((n, 128), jnp.float32) for n in lines],
        in_specs=[in_hbm] * 6 + [in_vmem],
        out_specs=[in_vmem] * 9,
        scratch_shapes=[
            pltpu.VMEM(down.shape, jnp.float32),
            pltpu.VMEM(mixed.shape, jnp.float32),
            pltpu.VMEM((5, N, N, 16, 128), jnp.float32),
            pltpu.SemaphoreType.DMA,
            pltpu.SemaphoreType.DMA((2,)),
        ],
    )(split[0], down, *split[1:], mixed, norm)


def merge_body(at, near, far, half, out):
    out[...] = near[...] + far[...]
    rows = pl.ds(at, half.shape[0])
    out[rows] += half[...]


def merge(at, *parts):
    return pl.pallas_call(
        functools.partial(merge_body, at),
        name="merge",
        compiler_params=pltpu.CompilerParams(vmem_limit_bytes=8 << 20),
        out_shape=pltpu.VMEM((ROWS, 128), jnp.float32),
        in_specs=[in_vmem] * 3,
        out_specs=in_vmem,
    )(*parts)


def middle_body(own, a, b, c, d, out):
    for t in range(T):
        rows = pl.ds(t * 128, 128)
        total = (own[rows] + a[rows]) + (b[rows] + c[rows]) + d[rows]
        out[:, t * 16 : (t + 1) * 16, :] = total.reshape(N, 16, 128)
    rows = pl.ds(T * 128, 8)
    norm = (own[rows] + a[rows]) + (b[rows] + c[rows]) + d[rows]
    out[:, T * 16 :, :] = jnp.broadcast_to(norm[None], (N, 8, 128))


def middle(*parts):
    return pl.pallas_call(
        middle_body,
        name="middle",
        compiler_params=pltpu.CompilerParams(vmem_limit_bytes=10 << 20),
        out_shape=pltpu.VMEM((N, PART, 128), jnp.float32),
        in_specs=[in_vmem] * 5,
        out_specs=in_vmem,
    )(*parts)


def update_body(got, up, down, q, k, v, mixed, norm, n_up, n_down, n_q, n_k, n_v, n_mixed, n_norm, copies):
    def step(t, weight):
        rows = pl.ds(t * 16, 16)
        total = got[0, rows]
        for s in range(1, N):
            total += got[s, rows]
        new = weight - learn_rate * (total * mean_rate)
        copies[:, rows] = jnp.broadcast_to(new.astype(jnp.bfloat16)[None], (N, 16, 128))
        return new

    for t in range(4):
        lanes = slice(t * 128, (t + 1) * 128)
        n_up[:, lanes] = step(t, up[:, lanes])
        n_down[:, lanes] = step(4 + t, down[:, lanes])
    n_q[...] = step(8, q[...])
    n_k[...] = step(9, k[...])
    n_v[...] = step(10, v[...])
    n_mixed[...] = step(11, mixed[...])
    total = got[0, T * 16 :]
    for s in range(1, N):
        total += got[s, T * 16 :]
    b = lax.axis_index("batch")
    z, y = b // N, b % N
    weight = pltpu.roll(norm[...], y * 16, 1)
    new = weight - learn_rate * (total * mean_rate)
    new = jnp.where(lax.broadcasted_iota(jnp.int32, (8, 128), 0) == z, new, 0.0)
    new = jnp.where(lax.broadcasted_iota(jnp.int32, (8, 128), 1) // 16 == y, new, 0.0)
    n_norm[...] = pltpu.roll(jnp.broadcast_to(jnp.sum(new, axis=0, keepdims=True), (8, 128)), 128 - y * 16, 1)
    copies[:, T * 16 :] = jnp.broadcast_to(new.astype(jnp.bfloat16)[None], (N, 8, 128))


def update(got, weights):
    shapes = [jax.ShapeDtypeStruct(w.shape, jnp.float32) for w in weights]
    return pl.pallas_call(
        update_body,
        name="update",
        compiler_params=pltpu.CompilerParams(vmem_limit_bytes=6 << 20),
        out_shape=shapes + [pltpu.VMEM((N, PART, 128), jnp.bfloat16)],
        in_specs=[in_vmem] * 8,
        out_specs=[in_vmem] * 8,
    )(got, *weights)


def unpack_body(own, a1, b1, a2, b2, a3, b3, h0, h1, up, down, q, k, v, mixed, norm, turned):
    c, pos, _ = place()
    chunks = {0: own, -1: a1, 1: b1, -2: a2, 2: b2, -3: a3, 3: b3}
    total = jnp.zeros((8, 128), jnp.float32)
    for d in range(-3, 5):
        f = (pos + d + N) % N
        for s in range(N):
            src, at = (chunks[d], s * PART) if d < 4 else (h0, s * PART) if s < 4 else (h1, (s - 4) * PART)
            z, y = jnp.where(c == 0, s, f), jnp.where(c == 0, f, s)
            for t in range(T):
                block = src[at + t * 16 : at + (t + 1) * 16]
                if t < 4:
                    up[z, y, :, t * 128 : (t + 1) * 128] = block
                elif t < 8 or t == 11:
                    turned[t - 4 if t < 8 else 4, z, y] = block
                else:
                    (q, k, v)[t - 8][z, y] = block
            total += src[at + T * 16 : at + PART].astype(jnp.float32)
    norm[...] = total.astype(jnp.bfloat16)
    for dst, t0, n in ((down, 0, 4), (mixed, 4, 1)):
        for z in range(N):
            for t in range(n):
                dst[t * 128 : (t + 1) * 128, z * 128 : (z + 1) * 128] = turned[t0 + t, z].reshape(128, 128).T


def unpack(*chunks):
    def out(*shape):
        return jax.ShapeDtypeStruct(shape, jnp.bfloat16)

    up, down, q, k, v, mixed, norm = pl.pallas_call(
        unpack_body,
        name="unpack",
        compiler_params=pltpu.CompilerParams(vmem_limit_bytes=16 << 20),
        out_shape=[out(N, N, 16, 512), out(512, 1024)] + [out(N, N, 16, 128)] * 3 + [out(128, 1024), out(8, 128)],
        in_specs=[in_vmem] * 9,
        out_specs=[in_vmem] * 7,
        scratch_shapes=[pltpu.VMEM((5, N, N, 16, 128), jnp.bfloat16)],
    )(*chunks)
    flat = [a.reshape(1024, -1) for a in (up, q, k, v)]
    return flat[0], down, *flat[1:], mixed, norm.reshape(1024)


def summed(chunks):
    own, p1, m1, p2, m2, p3, m3, h0, h1 = chunks
    far_p, far_m = shift(p3, 1), shift(m3, -1)
    half_p, half_m = shift(h0, 2), shift(h1, -2)
    near_p, near_m = shift(p1, 1), shift(m1, -1)
    to_p, to_m = merge(0, p2, far_p, half_p), merge(HALF, m2, far_m, half_m)
    return middle(own, near_p, near_m, shift(to_p, 2), shift(to_m, -2))


def spread(own):
    half = own.shape[0] // 2
    a2, b2 = shift(own, 2), shift(own, -2)
    a1, b1 = shift(own, 1), shift(own, -1)
    a3, b3 = shift(a2, 1), shift(b2, -1)
    h0, h1 = shift(a2[:half], 2), shift(b2[half:], -2)
    return own, a1, b1, a2, b2, a3, b3, h0, h1


def shards(g_up, g_down, g_q, g_k, g_v, g_mixed, g_norm, up, down, q, k, v, mixed, norm):
    chunks = pack(g_up[0], g_down[0], g_q[0], g_k[0], g_v[0], g_mixed[0], g_norm.reshape(8, 128))
    norm_tile = jnp.broadcast_to(jnp.pad(norm, (0, 112)), (8, 128))
    parts, norm_tile = lax.optimization_barrier((summed(chunks), norm_tile))
    got = exchange(parts, True)
    *new, mine = update(got, (up, down.T, q, k, v, mixed.T, norm_tile))
    copies = unpack(*spread(exchange(mine, True).reshape(N * PART, 128)))
    n_up, n_down, n_q, n_k, n_v, n_mixed, n_norm = new
    return (*copies, n_up, n_down.T, n_q, n_k, n_v, n_mixed.T, n_norm[0, :16])


def solution(mesh):
    placed = (
        P("batch", None, "cols"),
        P("batch", "cols", None),
        P("batch", None, "cols"),
        P("batch", None, "cols"),
        P("batch", None, "cols"),
        P("batch", "cols", None),
        P("batch", None),
        P("batch", "cols"),
        P("cols", "batch"),
        P("batch", "cols"),
        P("batch", "cols"),
        P("batch", "cols"),
        P("cols", "batch"),
        P("batch"),
    )
    whole = (P(None, "cols"), P("cols", None), P(None, "cols"), P(None, "cols"), P(None, "cols"), P("cols", None), P())
    return jax.shard_map(shards, mesh=mesh, in_specs=placed, out_specs=whole + placed[7:], check_vma=False)
```
